32 devices in a mesh: elem: 8 (over z, core), lev: 4 (over y, x).
Axes of the slice: x: 2, y: 2, z: 4, core: 2. Of those that a mesh axis runs over, the one named last changes fastest.
Arguments:
- tracers: float32 [512, 16, 640], P('elem', 'lev'), may hold values from 0.1 to 120, as said below
- ref_index: int32 [512, 16], P('elem'), may hold values from 0 to 63
- requests: int32 [8, 2, 16], P('elem'), may hold values from -1 to 63, as said below
- source: int32 [512], P('elem'), may hold values from 0 to 95, as said below
- target_mean: float32 [40], replicated, may hold values from 0.5 to 5
Outputs:
- transported: float32 [512, 16, 640], P('elem', 'lev')
The draws below stay inside these ranges and needn't reach their ends.
Inputs may be any that keep to these rules, and one draw needn't show every extreme that they name: Row 0 of requests[d] holds distinct element indices of block d - 1 (wrapping), row 1 of block d + 1; the valid entries come first and the rest are -1; every row holds 1 to 16 valid entries and some row holds exactly 16. `source`: every slot names an own element (below 64) or a valid entry of the block's requests: 64 + k for row 0, 80 + k for row 1. `tracers`: all entries are positive.
All inputs are finite; a program needn't handle non-finite values.
Results may differ from the reference program's by a relative error of at most 0.0003.
Values sent between devices are 32-bit elements; how exact they have to be, the bound alone decides.
A program may use at most 64 MiB of HBM per device.

```python
import math
import jax
import jax.numpy as jnp
from jax import lax

TR = 40
NPTS = 16
REFS = 64
ELEM_DEV = 64
SLOTS = 16
NELEM = 512
NLEV = 16
N_ELEM = 8


def routing(key):
    key = jax.random.fold_in(key, 17)
    key_count, key_band, key_busy, key_perm, key_side, key_left, key_right, key_near, key_high = jax.random.split(key, 9)
    low_counts = jax.random.randint(key_count, (N_ELEM, 2), 1, max(SLOTS // 3, 1) + 1)
    high_counts = jax.random.randint(key_high, (N_ELEM, 2), max(SLOTS // 2, 1), SLOTS + 1)
    band_start = jax.random.randint(key_band, (), 0, N_ELEM)
    in_band = (jnp.arange(N_ELEM, dtype=jnp.int32) - band_start) % N_ELEM < max(N_ELEM // 8, 1)
    counts = jnp.where(in_band[:, None], high_counts, low_counts)
    busiest = jax.random.randint(key_busy, (), 0, N_ELEM * 2)
    flat_counts = jnp.where(jnp.arange(N_ELEM * 2, dtype=jnp.int32) == busiest, SLOTS, counts.reshape(-1))
    counts = flat_counts.reshape(N_ELEM, 2)
    row_keys = jax.random.split(key_perm, N_ELEM * 2)

    def choose(one_key):
        return jax.random.permutation(one_key, ELEM_DEV)[:SLOTS]
    element_ids = jax.vmap(choose)(row_keys).reshape(N_ELEM, 2, SLOTS).astype(jnp.int32)
    usable = jnp.arange(SLOTS, dtype=jnp.int32)[None, None, :] < counts[:, :, None]
    requests = jnp.where(usable, element_ids, -1).astype(jnp.int32)
    position = jnp.arange(NELEM, dtype=jnp.int32) % ELEM_DEV
    device = jnp.arange(NELEM, dtype=jnp.int32) // ELEM_DEV
    branch_pick = jax.random.randint(key_side, (NELEM,), 0, 4)
    nearby = jnp.clip(position + jax.random.randint(key_near, (NELEM,), -2, 3), 0, ELEM_DEV - 1)
    left_slot = ELEM_DEV + jax.random.randint(key_left, (NELEM,), 0, counts[device, 0])
    right_slot = ELEM_DEV + SLOTS + jax.random.randint(key_right, (NELEM,), 0, counts[device, 1])
    use_left = (position < ELEM_DEV // 4) & (branch_pick < 2)
    use_right = (position >= ELEM_DEV - ELEM_DEV // 4) & (branch_pick < 2)
    source = jnp.where(use_left, left_slot, jnp.where(use_right, right_slot, nearby)).astype(jnp.int32)
    return (requests, source)


def draw_requests(key, part):
    return routing(key)[0]


def draw_source(key, part):
    return routing(key)[1]


def draw_tracers(key, part):
    key = jax.random.fold_in(key, 29)
    shape = (NELEM, NLEV, TR * NPTS)
    elem_frac = (jnp.arange(NELEM, dtype=jnp.float32) / NELEM)[:, None, None]
    lev_frac = (jnp.arange(NLEV, dtype=jnp.float32) / NLEV)[None, :, None]
    base = jnp.exp(jax.random.uniform(key, shape, jnp.float32, math.log(0.1), math.log(10.0)))
    rising = (1.0 + elem_frac) * (1.0 + 0.5 * lev_frac)
    return (base * rising).astype(jnp.float32)


def plant(values, key, least, top_value):
    spot = [jax.random.randint(jax.random.fold_in(key, axis), (), 0, length) for axis, length in enumerate(values.shape)]
    main_axis = values.shape.index(max(values.shape))
    neighbour = spot[:main_axis] + [(spot[main_axis] + 1) % values.shape[main_axis]] + spot[main_axis + 1:]
    return values.at[tuple(spot)].set(least).at[tuple(neighbour)].set(top_value)


def setup_inputs(seed: int = 0) -> dict:
    arg_keys = jax.random.split(jax.random.key(seed), 6)
    tracers = draw_tracers(jax.random.fold_in(arg_keys[5], 71), 0)
    ref_index = plant(jax.random.randint(arg_keys[1], (NELEM, NPTS), 0, REFS), jax.random.fold_in(arg_keys[1], 1), 0, REFS - 1).astype(jnp.int32)
    requests = draw_requests(jax.random.fold_in(arg_keys[5], 71), 0)
    source = draw_source(jax.random.fold_in(arg_keys[5], 71), 0)
    target_mean = jnp.clip(jnp.exp(jax.random.uniform(arg_keys[4], (TR,), jnp.float32, math.log(0.5), math.log(5.0))), 0.5, 5.0)
    return {"tracers": tracers, "ref_index": ref_index, "requests": requests, "source": source, "target_mean": target_mean}


def lagrange_table():
    side = math.isqrt(REFS)
    gll_nodes = [-1.0, -math.sqrt(0.2), math.sqrt(0.2), 1.0]
    points = -1.0 + 2.0 * jnp.arange(side, dtype=jnp.float32) / (side - 1)
    columns = []
    for which in range(4):
        basis = jnp.ones((side,), jnp.float32)
        for other in range(4):
            if other != which:
                basis = basis * (points - gll_nodes[other]) / (gll_nodes[which] - gll_nodes[other])
        columns.append(basis)
    one_dim = jnp.stack(columns, axis=1)
    return (one_dim[:, None, :, None] * one_dim[None, :, None, :]).reshape(side * side, 16)

def quadrature():
    edge = jnp.array([1.0 / 6.0, 5.0 / 6.0, 5.0 / 6.0, 1.0 / 6.0], jnp.float32)
    return (edge[:, None] * edge[None, :]).reshape(16)

def interpolate(source_rows, ref_index):
    elem_count, levels, width = source_rows.shape
    onehot = (ref_index[:, :, None] == jnp.arange(REFS, dtype=jnp.int32)[None, None, :]).astype(jnp.float32)
    matrix = jnp.einsum('epr,rn->epn', onehot, lagrange_table(), precision=lax.Precision.HIGHEST)
    values = source_rows.reshape(elem_count, levels * (width // 16), 16)
    result = jnp.einsum('epn,ecn->ecp', matrix, values, precision=lax.Precision.HIGHEST)
    lowest = lax.optimization_barrier(jnp.min(values, axis=2, keepdims=True))
    highest = lax.optimization_barrier(jnp.max(values, axis=2, keepdims=True))
    result = jnp.minimum(jnp.maximum(result, lowest), highest)
    return result.reshape(elem_count, levels, width)

def reference(tracers, ref_index, requests, source, target_mean):

    def block(device):
        first_row = device * ELEM_DEV
        left_dev = (device + N_ELEM - 1) % N_ELEM
        right_dev = (device + 1) % N_ELEM
        slots_here = lax.dynamic_slice_in_dim(source, first_row, ELEM_DEV, 0)
        refs_here = lax.dynamic_slice_in_dim(ref_index, first_row, ELEM_DEV, 0)
        wanted = requests[device]
        own_global = first_row + jnp.arange(ELEM_DEV, dtype=jnp.int32)
        left_global = left_dev * ELEM_DEV + jnp.maximum(wanted[0], 0)
        right_global = right_dev * ELEM_DEV + jnp.maximum(wanted[1], 0)
        slot_global = jnp.concatenate([own_global, left_global, right_global]).astype(jnp.int32)
        source_rows = tracers[slot_global[slots_here]]
        return interpolate(source_rows, refs_here)
    clipped = lax.map(block, jnp.arange(N_ELEM, dtype=jnp.int32))
    clipped = clipped.reshape(NELEM, NLEV, TR, NPTS)
    mass = jnp.einsum('eltn,n->t', clipped, quadrature(), precision=lax.Precision.HIGHEST)
    factor = target_mean * (4.0 * NELEM * NLEV) / mass
    return (clipped * factor[None, None, :, None]).reshape(NELEM, NLEV, TR * NPTS)
```

```python
import functools
import math

import jax
import jax.numpy as jnp
from jax import lax
from jax.experimental import pallas as pl
from jax.experimental.pallas import tpu as pltpu
from jax.sharding import PartitionSpec as P

NPTS = 16
SIDE = 8
LANES = 128
UNROLL = 4
MESH = pl.DeviceIdType.MESH
NODES = [-1.0, -math.sqrt(0.2), math.sqrt(0.2), 1.0]


def basis(x):
    d = [x - g for g in NODES]
    scale = [1.0 / math.prod(NODES[i] - NODES[k] for k in range(4) if k != i) for i in range(4)]
    low, high = d[0] * d[1], d[2] * d[3]
    parts = [d[1] * high, d[0] * high, low * d[3], low * d[2]]
    return [p * s for p, s in zip(parts, scale)]


def permute(v, index):
    return jnp.take_along_axis(v, index, axis=1, mode="promise_in_bounds")


def kernel(ne, nl, nelem, levels, chunks, slots, *refs):
    x_hbm, reft_ref, req_ref, src_ref, tm_ref, clip_out, fac_out = refs[:7]
    tabs = refs[7 : 7 + chunks]
    (sendb, halo, gbuf, clipb, rows, coef, massb, mrecv, req_r, req_l,
     in_sem, out_sem, rq_send, rq_recv, h_send, h_recv, m_send, m_recv, e_sem, l_sem) = refs[7 + chunks :]
    me_e, me_l = lax.axis_index("elem"), lax.axis_index("lev")
    right, left = lax.rem(me_e + 1, ne), lax.rem(me_e + ne - 1, ne)
    pairs = nelem // 2
    lrounds = [1 << j for j in range(int(math.log2(nl)))]
    erounds = [1 << j for j in range(int(math.log2(ne)) - 1)]

    loads = [pltpu.make_async_copy(x_hbm.at[:, c], tabs[c].at[pl.ds(0, nelem)], in_sem.at[c]) for c in range(chunks)]

    def hello(sem, e, l):
        pl.semaphore_signal(sem, inc=1, device_id=(e, l), device_id_type=MESH)

    barrier = pltpu.get_barrier_semaphore()
    hello(barrier, right, me_l)
    hello(barrier, left, me_l)
    for d in lrounds:
        hello(barrier, me_e, me_l ^ d)
    for load in loads:
        load.start()
    pl.semaphore_wait(barrier, 2 + len(lrounds))

    def remote(src, dst, ssem, rsem, e, l):
        return pltpu.make_async_remote_copy(
            src_ref=src, dst_ref=dst, send_sem=ssem, recv_sem=rsem, device_id=(e, l), device_id_type=MESH
        )

    ask_l = remote(req_ref, req_r, rq_send.at[0], rq_recv.at[0], left, me_l)
    ask_r = remote(req_ref, req_l, rq_send.at[1], rq_recv.at[1], right, me_l)
    ask_l.start()
    ask_r.start()

    steps = []
    for j, d in enumerate(erounds):
        fwd, back = lax.rem(me_e + d, ne), lax.rem(me_e + ne - d, ne)
        steps.append((lambda j=j, f=fwd, b=back: (hello(e_sem.at[j], f, me_l), hello(e_sem.at[j], b, me_l)),
                      lambda j=j: pl.semaphore_wait(e_sem.at[j], 2)))
    for j, d in enumerate(lrounds):
        steps.append((lambda j=j, d=d: hello(l_sem.at[j], me_e, me_l ^ d),
                      lambda j=j: pl.semaphore_wait(l_sem.at[j], 1)))
    steps[0][0]()

    lane = lax.broadcasted_iota(jnp.int32, (8, LANES), 1)
    point = lane % NPTS
    hi, lo = point // 4, point % 4

    spread = (lax.broadcasted_iota(jnp.int32, (NPTS, LANES), 1) % NPTS
              == lax.broadcasted_iota(jnp.int32, (NPTS, LANES), 0)).astype(jnp.float32)
    refs_f = reft_ref[...].astype(jnp.float32)
    tiled = lax.dot_general(refs_f, spread, (((0,), (0,)), ((), ())), preferred_element_type=jnp.float32)
    rep = (lax.broadcasted_iota(jnp.int32, (nelem * 4, nelem), 0) // 4
           == lax.broadcasted_iota(jnp.int32, (nelem * 4, nelem), 1)).astype(jnp.float32)
    rows[...] = jnp.dot(rep, tiled, preferred_element_type=jnp.float32)

    def shuffle(parts, which):
        return [jnp.where(which == 0, parts[k], jnp.where(which == 1, parts[1 ^ k],
                jnp.where(which == 2, parts[2 ^ k], parts[3 ^ k]))) for k in range(4)]

    def fill(i, carry):
        for u in range(UNROLL):
            q = i * UNROLL + u
            r = rows[pl.ds(pl.multiple_of(q * 8, 8), 8), :]
            a = jnp.floor((r + 0.5) * (1.0 / SIDE))
            b = r - SIDE * a
            la = shuffle(basis(-1.0 + a * (2.0 / (SIDE - 1))), hi)
            lb = shuffle(basis(-1.0 + b * (2.0 / (SIDE - 1))), lo)
            for k in range(NPTS):
                coef[k, q] = la[k // 4] * lb[k % 4]
        return carry

    lax.fori_loop(0, pairs // UNROLL, fill, 0)

    if len(steps) > 1:
        steps[0][1]()
        steps[1][0]()
    at = 1

    ask_l.wait()
    ask_r.wait()
    sends = []
    wanted = [[jnp.maximum(req_r[0, s], 0) for s in range(slots)], [jnp.maximum(req_l[1, s], 0) for s in range(slots)]]
    for c in range(chunks):
        loads[c].wait()
        for side, to in ((0, right), (1, left)):
            for s in range(slots):
                sendb[c, side, s] = tabs[c][wanted[side][s]]
            copy = remote(sendb.at[c, side], halo.at[c, side], h_send.at[c, side], h_recv.at[c, side], to, me_l)
            copy.start()
            sends.append(copy)

    while at < len(steps):
        steps[at][1]()
        if at + 1 < len(steps):
            steps[at + 1][0]()
        at += 1

    index = [lane ^ k for k in range(NPTS)]
    totals, stores = [], []
    for c in range(chunks):
        for side in range(2):
            sends[2 * c + side].wait_recv()
            tabs[c][pl.ds(nelem + side * slots, slots)] = halo[c, side]
        for q in range(pairs):
            gbuf[c, q, 0:4] = tabs[c][src_ref[2 * q]]
            gbuf[c, q, 4:8] = tabs[c][src_ref[2 * q + 1]]

        def work(i, acc, c=c):
            qs = [i * UNROLL + u for u in range(UNROLL)]
            vs = [gbuf[c, q] for q in qs]
            low, high, out = list(vs), list(vs), [coef[0, q] * v for q, v in zip(qs, vs)]
            for k in range(1, NPTS):
                for u in range(UNROLL):
                    w = permute(vs[u], index[k])
                    out[u] = out[u] + coef[k, qs[u]] * w
                    if k < 4:
                        low[u], high[u] = jnp.minimum(low[u], w), jnp.maximum(high[u], w)
            for k in (4, 8):
                for u in range(UNROLL):
                    low[u] = jnp.minimum(low[u], permute(low[u], index[k]))
                    high[u] = jnp.maximum(high[u], permute(high[u], index[k]))
            for u in range(UNROLL):
                res = jnp.minimum(jnp.maximum(out[u], low[u]), high[u])
                clipb[c, 2 * qs[u]] = res[0:4]
                clipb[c, 2 * qs[u] + 1] = res[4:8]
                acc = acc + res
            return acc

        totals.append(lax.fori_loop(0, pairs // UNROLL, work, jnp.zeros((8, LANES), jnp.float32)))
        store = pltpu.make_async_copy(clipb.at[c], clip_out.at[:, c], out_sem.at[c])
        store.start()
        stores.append(store)

    edge = [1.0 / 6.0, 5.0 / 6.0]
    weight = jnp.where((hi == 0) | (hi == 3), edge[0], edge[1]) * jnp.where((lo == 0) | (lo == 3), edge[0], edge[1])
    row = lax.broadcasted_iota(jnp.int32, (8, LANES), 0)
    part = jnp.zeros((8, LANES), jnp.float32)
    for c in range(chunks):
        one = jnp.sum(totals[c], axis=0, keepdims=True)
        part = jnp.where(row == c, one, part)
    part = part * weight
    for k in (1, 2, 4, 8):
        part = part + permute(part, index[k])
    packed = jnp.sum(jnp.where(point == row, part, 0.0), axis=0, keepdims=True)
    massb[0] = packed

    count = ne * nl

    def tell(de):
        e = lax.rem(me_e + de, ne)
        for dl in range(nl):
            l = lax.rem(me_l + dl, nl)
            slot = de * nl + dl - 1
            if isinstance(de, int) and slot < 0:
                continue
            remote(massb.at[0], mrecv.at[slot], m_send, m_recv, e, l).start()

    def tell_loop(de, carry):
        tell(de)
        return carry

    if count <= 64:
        for de in range(ne):
            tell(de)
    else:
        tell(0)
        lax.fori_loop(1, ne, tell_loop, 0)

    tm = jnp.zeros((8, LANES), jnp.float32)
    group = row * (LANES // NPTS) + lane // NPTS
    for t in range(chunks * LANES // NPTS):
        tm = jnp.where(group == t, tm_ref[t], tm)
    tm = tm * (4.0 * nelem * ne * levels * nl)
    for copy in sends:
        copy.wait_send()
    for store in stores:
        store.wait()
    everyone = remote(mrecv, mrecv, m_send, m_recv, right, me_l)
    everyone.wait_recv()
    mass = packed
    if count <= 64:
        for s in range(count - 1):
            mass = mass + mrecv[s]
    else:
        mass = lax.fori_loop(0, count - 1, lambda s, m: m + mrecv[s], mass)
    full = permute(jnp.broadcast_to(mass, (8, LANES)), (lane // NPTS) * NPTS + row)
    fac_out[...] = tm / full
    everyone.wait_send()


def per_device(ne, nl, tracers, ref_index, requests, source, target_mean):
    nelem, levels, width = tracers.shape
    chunks = width // LANES
    slots = requests.shape[2]
    x = tracers.reshape(nelem, levels, chunks, LANES).transpose(0, 2, 1, 3)
    f32 = jnp.float32
    vm = lambda *s: pltpu.VMEM(s, f32)
    dma = lambda *s: pltpu.SemaphoreType.DMA(s)
    smem, any_, vmem = (pl.BlockSpec(memory_space=m) for m in (pltpu.SMEM, pl.ANY, pltpu.VMEM))
    clipped, factor = pl.pallas_call(
        functools.partial(kernel, ne, nl, nelem, levels, chunks, slots),
        out_shape=(jax.ShapeDtypeStruct((nelem, chunks, levels, LANES), f32), jax.ShapeDtypeStruct((8, LANES), f32)),
        in_specs=[any_, vmem, smem, smem, smem],
        out_specs=(any_, vmem),
        scratch_shapes=[vm(nelem + 2 * slots, levels, LANES) for _ in range(chunks)] + [
            vm(chunks, 2, slots, levels, LANES),
            vm(chunks, 2, slots, levels, LANES),
            vm(chunks, nelem // 2, 8, LANES),
            vm(chunks, nelem, levels, LANES),
            vm(nelem * levels, LANES),
            vm(NPTS, nelem // 2, 8, LANES),
            vm(1, 1, LANES),
            vm(ne * nl - 1, 1, LANES),
            pltpu.SMEM((2, slots), jnp.int32),
            pltpu.SMEM((2, slots), jnp.int32),
            dma(chunks), dma(chunks), dma(2), dma(2), dma(chunks, 2), dma(chunks, 2),
            pltpu.SemaphoreType.DMA, pltpu.SemaphoreType.DMA,
            pltpu.SemaphoreType.REGULAR((max(int(math.log2(ne)) - 1, 1),)),
            pltpu.SemaphoreType.REGULAR((max(int(math.log2(nl)), 1),)),
        ],
        compiler_params=pltpu.CompilerParams(collective_id=0, has_side_effects=True),
    )(x, ref_index.T, requests[0], source, target_mean)
    out = clipped * factor[:chunks][None, :, None, :]
    return out.transpose(0, 2, 1, 3).reshape(nelem, levels, width)


def solution(mesh):
    placed = (P("elem", "lev", None), P("elem", None), P("elem", None, None), P("elem"), P())
    return jax.shard_map(
        functools.partial(per_device, mesh.shape["elem"], mesh.shape["lev"]),
        mesh=mesh, in_specs=placed, out_specs=P("elem", "lev", None), check_vma=False,
    )
```

```python
import functools
import math

import jax
import jax.numpy as jnp
from jax import lax
from jax.experimental import pallas as pl
from jax.experimental.pallas import tpu as pltpu
from jax.sharding import PartitionSpec as P

NPTS = 16
SIDE = 8
LANES = 128
MESH = pl.DeviceIdType.MESH
NODES = [-1.0, -math.sqrt(0.2), math.sqrt(0.2), 1.0]


def basis(x):
    d = [x - g for g in NODES]
    scale = [1.0 / math.prod(NODES[i] - NODES[k] for k in range(4) if k != i) for i in range(4)]
    low, high = d[0] * d[1], d[2] * d[3]
    parts = [d[1] * high, d[0] * high, low * d[3], low * d[2]]
    return [p * s for p, s in zip(parts, scale)]


def permute(v, index):
    return jnp.take_along_axis(v, index, axis=1, mode="promise_in_bounds")


def kernel(ne, nl, nelem, levels, chunks, slots, *refs):
    x_hbm, reft_ref, req_ref, src_ref, tm_ref, clip_out, fac_out = refs[:7]
    (tab, sendb, halo, gbuf, turned, clipb, coef, massb, mrecv, req_r, req_l,
     in_sem, out_sem, rq_send, rq_recv, h_send, h_recv, m_send, m_recv, e_sem, l_sem) = refs[7:]
    me_e, me_l = lax.axis_index("elem"), lax.axis_index("lev")
    right, left = lax.rem(me_e + 1, ne), lax.rem(me_e + ne - 1, ne)
    halves = nelem * levels // LANES
    each = nelem // halves
    lrounds = [1 << j for j in range(int(math.log2(nl)))]
    erounds = [1 << j for j in range(int(math.log2(ne)) - 1)]

    loads = [pltpu.make_async_copy(x_hbm.at[:, c], tab.at[c, pl.ds(0, nelem)], in_sem.at[c]) for c in range(chunks)]

    def hello(sem, e, l):
        pl.semaphore_signal(sem, inc=1, device_id=(e, l), device_id_type=MESH)

    barrier = pltpu.get_barrier_semaphore()
    hello(barrier, right, me_l)
    hello(barrier, left, me_l)
    for d in lrounds:
        hello(barrier, me_e, me_l ^ d)
    for load in loads:
        load.start()
    pl.semaphore_wait(barrier, 2 + len(lrounds))

    def remote(src, dst, ssem, rsem, e, l):
        return pltpu.make_async_remote_copy(
            src_ref=src, dst_ref=dst, send_sem=ssem, recv_sem=rsem, device_id=(e, l), device_id_type=MESH
        )

    ask_l = remote(req_ref, req_r, rq_send.at[0], rq_recv.at[0], left, me_l)
    ask_r = remote(req_ref, req_l, rq_send.at[1], rq_recv.at[1], right, me_l)
    ask_l.start()
    ask_r.start()

    steps = []
    for j, d in enumerate(erounds):
        fwd, back = lax.rem(me_e + d, ne), lax.rem(me_e + ne - d, ne)
        steps.append((lambda j=j, f=fwd, b=back: (hello(e_sem.at[j], f, me_l), hello(e_sem.at[j], b, me_l)),
                      lambda j=j: pl.semaphore_wait(e_sem.at[j], 2)))
    for j, d in enumerate(lrounds):
        steps.append((lambda j=j, d=d: hello(l_sem.at[j], me_e, me_l ^ d),
                      lambda j=j: pl.semaphore_wait(l_sem.at[j], 1)))
    steps[0][0]()

    lane = lax.broadcasted_iota(jnp.int32, (8, LANES), 1)
    point = lane % NPTS
    hi, lo = point // 4, point % 4

    refs_f = reft_ref[...].astype(jnp.float32)
    rep = (lax.broadcasted_iota(jnp.int32, (nelem, nelem * levels), 1) // levels
           == lax.broadcasted_iota(jnp.int32, (nelem, nelem * levels), 0)).astype(jnp.float32)
    spread = jnp.dot(refs_f, rep, preferred_element_type=jnp.float32)
    for h in range(halves):
        r = spread[:, h * LANES : (h + 1) * LANES]
        a = jnp.floor((r + 0.5) * (1.0 / SIDE))
        b = r - SIDE * a
        la = basis(-1.0 + a * (2.0 / (SIDE - 1)))
        lb = basis(-1.0 + b * (2.0 / (SIDE - 1)))
        for n in range(NPTS):
            coef[h, n] = la[n // 4] * lb[n % 4]

    if len(steps) > 1:
        steps[0][1]()
        steps[1][0]()
    at = 1

    ask_l.wait()
    ask_r.wait()
    for load in loads:
        load.wait()
    wanted = [[jnp.maximum(req_r[0, s], 0) for s in range(slots)], [jnp.maximum(req_l[1, s], 0) for s in range(slots)]]

    def rows_to(c, side):
        to = left if side else right
        return remote(sendb.at[c, side], halo.at[c, side], h_send.at[c, side], h_recv.at[c, side], to, me_l)

    for c in range(chunks):
        for side in range(2):
            for s in range(slots):
                sendb[c, side, s] = tab[c, wanted[side][s]]
            rows_to(c, side).start()

    while at < len(steps):
        steps[at][1]()
        if at + 1 < len(steps):
            steps[at + 1][0]()
        at += 1

    index = [lane ^ k for k in range(NPTS)]
    row = lax.broadcasted_iota(jnp.int32, (8, LANES), 0)
    store = lambda c: pltpu.make_async_copy(clipb.at[c], clip_out.at[:, c], out_sem.at[c])

    def work(c, part):
        for side in range(2):
            rows_to(c, side).wait_recv()
            tab[c, pl.ds(nelem + side * slots, slots)] = halo[c, side]
        total = jnp.zeros((LANES, LANES), jnp.float32)
        for h in range(halves):
            for q in range(each):
                gbuf[h, q * levels : (q + 1) * levels] = tab[c, src_ref[h * each + q]]
            turned[h] = gbuf[h].T
            done = []
            for t in range(LANES // NPTS):
                v = turned[h, t * NPTS : (t + 1) * NPTS]
                low, high = jnp.min(v, axis=0, keepdims=True), jnp.max(v, axis=0, keepdims=True)
                out = jnp.zeros((NPTS, LANES), jnp.float32)
                for n in range(NPTS):
                    out = out + coef[h, n] * turned[h, t * NPTS + n : t * NPTS + n + 1]
                done.append(jnp.minimum(jnp.maximum(out, low), high))
            back = jnp.concatenate(done, axis=0).T
            clipb[c, h * each : (h + 1) * each] = back.reshape(each, levels, LANES)
            total = total + back
        store(c).start()
        return jnp.where(row == c, jnp.sum(total, axis=0, keepdims=True), part)

    part = lax.fori_loop(0, chunks, work, jnp.zeros((8, LANES), jnp.float32))

    edge = [1.0 / 6.0, 5.0 / 6.0]
    weight = jnp.where((hi == 0) | (hi == 3), edge[0], edge[1]) * jnp.where((lo == 0) | (lo == 3), edge[0], edge[1])
    part = part * weight
    for k in (1, 2, 4, 8):
        part = part + permute(part, index[k])
    packed = jnp.sum(jnp.where(point == row, part, 0.0), axis=0, keepdims=True)
    massb[0] = packed

    count = ne * nl

    def tell(de):
        e = lax.rem(me_e + de, ne)
        for dl in range(nl):
            l = lax.rem(me_l + dl, nl)
            slot = de * nl + dl - 1
            if isinstance(de, int) and slot < 0:
                continue
            remote(massb.at[0], mrecv.at[slot], m_send, m_recv, e, l).start()

    def tell_loop(de, carry):
        tell(de)
        return carry

    if count <= 64:
        for de in range(ne):
            tell(de)
    else:
        tell(0)
        lax.fori_loop(1, ne, tell_loop, 0)

    tm = jnp.zeros((8, LANES), jnp.float32)
    group = row * (LANES // NPTS) + lane // NPTS
    for t in range(chunks * LANES // NPTS):
        tm = jnp.where(group == t, tm_ref[t], tm)
    tm = tm * (4.0 * nelem * ne * levels * nl)
    for c in range(chunks):
        for side in range(2):
            rows_to(c, side).wait_send()
        store(c).wait()
    everyone = remote(mrecv, mrecv, m_send, m_recv, right, me_l)
    everyone.wait_recv()
    mass = packed
    if count <= 64:
        for s in range(count - 1):
            mass = mass + mrecv[s]
    else:
        mass = lax.fori_loop(0, count - 1, lambda s, m: m + mrecv[s], mass)
    full = permute(jnp.broadcast_to(mass, (8, LANES)), (lane // NPTS) * NPTS + row)
    fac_out[...] = tm / full
    everyone.wait_send()


def per_device(ne, nl, tracers, ref_index, requests, source, target_mean):
    nelem, levels, width = tracers.shape
    chunks = width // LANES
    slots = requests.shape[2]
    x = tracers.reshape(nelem, levels, chunks, LANES).transpose(0, 2, 1, 3)
    f32 = jnp.float32
    vm = lambda *s: pltpu.VMEM(s, f32)
    dma = lambda *s: pltpu.SemaphoreType.DMA(s)
    smem, any_, vmem = (pl.BlockSpec(memory_space=m) for m in (pltpu.SMEM, pl.ANY, pltpu.VMEM))
    clipped, factor = pl.pallas_call(
        functools.partial(kernel, ne, nl, nelem, levels, chunks, slots),
        out_shape=(jax.ShapeDtypeStruct((nelem, chunks, levels, LANES), f32), jax.ShapeDtypeStruct((8, LANES), f32)),
        in_specs=[any_, vmem, smem, smem, smem],
        out_specs=(any_, vmem),
        scratch_shapes=[
            vm(chunks, nelem + 2 * slots, levels, LANES),
            vm(chunks, 2, slots, levels, LANES),
            vm(chunks, 2, slots, levels, LANES),
            vm(nelem * levels // LANES, LANES, LANES),
            vm(nelem * levels // LANES, LANES, LANES),
            vm(chunks, nelem, levels, LANES),
            vm(nelem * levels // LANES, NPTS, NPTS, LANES),
            vm(1, 1, LANES),
            vm(ne * nl - 1, 1, LANES),
            pltpu.SMEM((2, slots), jnp.int32),
            pltpu.SMEM((2, slots), jnp.int32),
            dma(chunks), dma(chunks), dma(2), dma(2), dma(chunks, 2), dma(chunks, 2),
            pltpu.SemaphoreType.DMA, pltpu.SemaphoreType.DMA,
            pltpu.SemaphoreType.REGULAR((max(int(math.log2(ne)) - 1, 1),)),
            pltpu.SemaphoreType.REGULAR((max(int(math.log2(nl)), 1),)),
        ],
        compiler_params=pltpu.CompilerParams(collective_id=0, has_side_effects=True),
    )(x, ref_index.T, requests[0], source, target_mean)
    out = clipped * factor[:chunks][None, :, None, :]
    return out.transpose(0, 2, 1, 3).reshape(nelem, levels, width)


def solution(mesh):
    placed = (P("elem", "lev", None), P("elem", None), P("elem", None, None), P("elem"), P())
    return jax.shard_map(
        functools.partial(per_device, mesh.shape["elem"], mesh.shape["lev"]),
        mesh=mesh, in_specs=placed, out_specs=P("elem", "lev", None), check_vma=False,
    )
```

```python
import functools
import math

import jax
import jax.numpy as jnp
from jax import lax
from jax.experimental import pallas as pl
from jax.experimental.pallas import tpu as pltpu
from jax.sharding import PartitionSpec as P

NPTS = 16
SIDE = 8
LANES = 128
MESH = pl.DeviceIdType.MESH
NODES = [-1.0, -math.sqrt(0.2), math.sqrt(0.2), 1.0]


def basis(x):
    d = [x - g for g in NODES]
    scale = [1.0 / math.prod(NODES[i] - NODES[k] for k in range(4) if k != i) for i in range(4)]
    low, high = d[0] * d[1], d[2] * d[3]
    parts = [d[1] * high, d[0] * high, low * d[3], low * d[2]]
    return [p * s for p, s in zip(parts, scale)]


def permute(v, index):
    return jnp.take_along_axis(v, index, axis=1, mode="promise_in_bounds")


def kernel(ne, nl, nelem, levels, chunks, slots, *refs):
    x_hbm, reft_hbm, req_hbm, src_hbm, tm_hbm, clip_out, fac_out = refs[:7]
    (reft_ref, req_ref, src_ref, tm_ref, tab, sendb, halo, gbuf, turned, coef, massb, mrecv, req_r, req_l,
     in_sem, small, rq_send, rq_recv, h_send, h_recv, m_send, m_recv, e_sem, l_sem) = refs[7:]
    me_e, me_l = lax.axis_index("elem"), lax.axis_index("lev")
    right, left = lax.rem(me_e + 1, ne), lax.rem(me_e + ne - 1, ne)
    halves = nelem * levels // LANES
    each = nelem // halves
    lrounds = [1 << j for j in range(int(math.log2(nl)))]
    erounds = [1 << j for j in range(int(math.log2(ne)) - 1)]

    loads = [pltpu.make_async_copy(x_hbm.at[:, c], tab.at[c, pl.ds(0, nelem)], in_sem.at[c]) for c in range(chunks)]

    fetch = [pltpu.make_async_copy(a, b, small.at[i]) for i, (a, b) in enumerate(
        [(req_hbm, req_ref), (reft_hbm, reft_ref), (src_hbm, src_ref), (tm_hbm, tm_ref)])]

    def hello(sem, e, l):
        pl.semaphore_signal(sem, inc=1, device_id=(e, l), device_id_type=MESH)

    barrier = pltpu.get_barrier_semaphore()
    hello(barrier, right, me_l)
    hello(barrier, left, me_l)
    for d in lrounds:
        hello(barrier, me_e, me_l ^ d)
    for copy in fetch + loads:
        copy.start()
    fetch[0].wait()
    pl.semaphore_wait(barrier, 2 + len(lrounds))

    def remote(src, dst, ssem, rsem, e, l):
        return pltpu.make_async_remote_copy(
            src_ref=src, dst_ref=dst, send_sem=ssem, recv_sem=rsem, device_id=(e, l), device_id_type=MESH
        )

    ask_l = remote(req_ref, req_r, rq_send.at[0], rq_recv.at[0], left, me_l)
    ask_r = remote(req_ref, req_l, rq_send.at[1], rq_recv.at[1], right, me_l)
    ask_l.start()
    ask_r.start()

    steps = []
    for j, d in enumerate(erounds):
        fwd, back = lax.rem(me_e + d, ne), lax.rem(me_e + ne - d, ne)
        steps.append((lambda j=j, f=fwd, b=back: (hello(e_sem.at[j], f, me_l), hello(e_sem.at[j], b, me_l)),
                      lambda j=j: pl.semaphore_wait(e_sem.at[j], 2)))
    for j, d in enumerate(lrounds):
        steps.append((lambda j=j, d=d: hello(l_sem.at[j], me_e, me_l ^ d),
                      lambda j=j: pl.semaphore_wait(l_sem.at[j], 1)))
    steps[0][0]()

    lane = lax.broadcasted_iota(jnp.int32, (8, LANES), 1)
    point = lane % NPTS
    hi, lo = point // 4, point % 4

    fetch[1].wait()
    refs_f = reft_ref[...].astype(jnp.float32)
    rep = (lax.broadcasted_iota(jnp.int32, (nelem, nelem * levels), 1) // levels
           == lax.broadcasted_iota(jnp.int32, (nelem, nelem * levels), 0)).astype(jnp.float32)
    spread = jnp.dot(refs_f, rep, preferred_element_type=jnp.float32)
    for h in range(halves):
        r = spread[:, h * LANES : (h + 1) * LANES]
        a = jnp.floor((r + 0.5) * (1.0 / SIDE))
        b = r - SIDE * a
        la = basis(-1.0 + a * (2.0 / (SIDE - 1)))
        lb = basis(-1.0 + b * (2.0 / (SIDE - 1)))
        for n in range(NPTS):
            coef[h, n] = la[n // 4] * lb[n % 4]

    if len(steps) > 1:
        steps[0][1]()
        steps[1][0]()
    at = 1

    fetch[2].wait()
    fetch[3].wait()
    ask_l.wait()
    ask_r.wait()
    for load in loads:
        load.wait()
    wanted = [[jnp.maximum(req_r[0, s], 0) for s in range(slots)], [jnp.maximum(req_l[1, s], 0) for s in range(slots)]]

    def rows_to(c, side):
        to = left if side else right
        return remote(sendb.at[c, side], halo.at[c, side], h_send.at[c, side], h_recv.at[c, side], to, me_l)

    for c in range(chunks):
        for side in range(2):
            for s in range(slots):
                sendb[c, side, s] = tab[c, wanted[side][s]]
            rows_to(c, side).start()

    while at < len(steps):
        steps[at][1]()
        if at + 1 < len(steps):
            steps[at + 1][0]()
        at += 1

    index = [lane ^ k for k in range(NPTS)]
    row = lax.broadcasted_iota(jnp.int32, (8, LANES), 0)

    def work(c, part):
        for side in range(2):
            rows_to(c, side).wait_recv()
            tab[c, pl.ds(nelem + side * slots, slots)] = halo[c, side]
        total = jnp.zeros((LANES, LANES), jnp.float32)
        for h in range(halves):
            for q in range(each):
                gbuf[h, q * levels : (q + 1) * levels] = tab[c, src_ref[h * each + q]]
            turned[h] = gbuf[h].T
            done = []
            for t in range(LANES // NPTS):
                v = turned[h, t * NPTS : (t + 1) * NPTS]
                low, high = jnp.min(v, axis=0, keepdims=True), jnp.max(v, axis=0, keepdims=True)
                out = jnp.zeros((NPTS, LANES), jnp.float32)
                for n in range(NPTS):
                    out = out + coef[h, n] * turned[h, t * NPTS + n : t * NPTS + n + 1]
                done.append(jnp.minimum(jnp.maximum(out, low), high))
            back = jnp.concatenate(done, axis=0).T
            clip_out[h * each : (h + 1) * each, c] = back.reshape(each, levels, LANES)
            total = total + back
        return jnp.where(row == c, jnp.sum(total, axis=0, keepdims=True), part)

    part = lax.fori_loop(0, chunks, work, jnp.zeros((8, LANES), jnp.float32))

    edge = [1.0 / 6.0, 5.0 / 6.0]
    weight = jnp.where((hi == 0) | (hi == 3), edge[0], edge[1]) * jnp.where((lo == 0) | (lo == 3), edge[0], edge[1])
    part = part * weight
    for k in (1, 2, 4, 8):
        part = part + permute(part, index[k])
    packed = jnp.sum(jnp.where(point == row, part, 0.0), axis=0, keepdims=True)
    massb[0] = packed

    count = ne * nl

    def tell(de):
        e = lax.rem(me_e + de, ne)
        for dl in range(nl):
            l = lax.rem(me_l + dl, nl)
            slot = de * nl + dl - 1
            if isinstance(de, int) and slot < 0:
                continue
            remote(massb.at[0], mrecv.at[slot], m_send, m_recv, e, l).start()

    def tell_loop(de, carry):
        tell(de)
        return carry

    if count <= 64:
        for de in range(ne):
            tell(de)
    else:
        tell(0)
        lax.fori_loop(1, ne, tell_loop, 0)

    tm = jnp.zeros((8, LANES), jnp.float32)
    group = row * (LANES // NPTS) + lane // NPTS
    for t in range(chunks * LANES // NPTS):
        tm = jnp.where(group == t, tm_ref[t], tm)
    tm = tm * (4.0 * nelem * ne * levels * nl)
    for c in range(chunks):
        for side in range(2):
            rows_to(c, side).wait_send()
    everyone = remote(mrecv, mrecv, m_send, m_recv, right, me_l)
    everyone.wait_recv()
    mass = packed
    if count <= 64:
        for s in range(count - 1):
            mass = mass + mrecv[s]
    else:
        mass = lax.fori_loop(0, count - 1, lambda s, m: m + mrecv[s], mass)
    full = permute(jnp.broadcast_to(mass, (8, LANES)), (lane // NPTS) * NPTS + row)
    fac_out[...] = tm / full
    everyone.wait_send()


def per_device(ne, nl, tracers, ref_index, requests, source, target_mean):
    nelem, levels, width = tracers.shape
    chunks = width // LANES
    slots = requests.shape[2]
    x = tracers.reshape(nelem, levels, chunks, LANES).transpose(0, 2, 1, 3)
    f32 = jnp.float32
    vm = lambda *s: pltpu.VMEM(s, f32)
    dma = lambda *s: pltpu.SemaphoreType.DMA(s)
    hbm, vmem = (pl.BlockSpec(memory_space=m) for m in (pltpu.HBM, pltpu.VMEM))
    clipped, factor = pl.pallas_call(
        functools.partial(kernel, ne, nl, nelem, levels, chunks, slots),
        out_shape=(jax.ShapeDtypeStruct((nelem, chunks, levels, LANES), f32), jax.ShapeDtypeStruct((8, LANES), f32)),
        in_specs=[hbm] * 5,
        out_specs=(vmem, vmem),
        scratch_shapes=[
            pltpu.VMEM((NPTS, nelem), jnp.int32),
            pltpu.SMEM((2, slots), jnp.int32),
            pltpu.SMEM((nelem,), jnp.int32),
            pltpu.SMEM((chunks * LANES // NPTS,), f32),
            vm(chunks, nelem + 2 * slots, levels, LANES),
            vm(chunks, 2, slots, levels, LANES),
            vm(chunks, 2, slots, levels, LANES),
            vm(nelem * levels // LANES, LANES, LANES),
            vm(nelem * levels // LANES, LANES, LANES),
            vm(nelem * levels // LANES, NPTS, NPTS, LANES),
            vm(1, 1, LANES),
            vm(ne * nl - 1, 1, LANES),
            pltpu.SMEM((2, slots), jnp.int32),
            pltpu.SMEM((2, slots), jnp.int32),
            dma(chunks), dma(4), dma(2), dma(2), dma(chunks, 2), dma(chunks, 2),
            pltpu.SemaphoreType.DMA, pltpu.SemaphoreType.DMA,
            pltpu.SemaphoreType.REGULAR((max(int(math.log2(ne)) - 1, 1),)),
            pltpu.SemaphoreType.REGULAR((max(int(math.log2(nl)), 1),)),
        ],
        compiler_params=pltpu.CompilerParams(collective_id=0, has_side_effects=True, vmem_limit_bytes=8 * 2**20),
    )(x, ref_index.T, requests[0], source, target_mean)
    out = clipped * factor[:chunks][None, :, None, :]
    return out.transpose(0, 2, 1, 3).reshape(nelem, levels, width)


def solution(mesh):
    placed = (P("elem", "lev", None), P("elem", None), P("elem", None, None), P("elem"), P())
    return jax.shard_map(
        functools.partial(per_device, mesh.shape["elem"], mesh.shape["lev"]),
        mesh=mesh, in_specs=placed, out_specs=P("elem", "lev", None), check_vma=False,
    )
```

```python
import functools
import math

import jax
import jax.numpy as jnp
from jax import lax
from jax.experimental import pallas as pl
from jax.experimental.pallas import tpu as pltpu
from jax.sharding import PartitionSpec as P

NPTS = 16
SIDE = 8
LANES = 128
MESH = pl.DeviceIdType.MESH
NODES = [-1.0, -math.sqrt(0.2), math.sqrt(0.2), 1.0]


def basis(x):
    d = [x - g for g in NODES]
    scale = [1.0 / math.prod(NODES[i] - NODES[k] for k in range(4) if k != i) for i in range(4)]
    low, high = d[0] * d[1], d[2] * d[3]
    parts = [d[1] * high, d[0] * high, low * d[3], low * d[2]]
    return [p * s for p, s in zip(parts, scale)]


def permute(v, index):
    return jnp.take_along_axis(v, index, axis=1, mode="promise_in_bounds")


def kernel(ne, nl, nelem, levels, chunks, slots, *refs):
    x_hbm, reft_hbm, req_hbm, src_hbm, tm_hbm, clip_out, fac_out = refs[:7]
    (reft_ref, req_ref, src_ref, tm_ref, tab, sendb, halo, gbuf, turned, coef, massb, mrecv, req_r, req_l,
     in_sem, small, rq_send, rq_recv, h_send, h_recv, m_send, m_recv, e_sem, l_sem) = refs[7:]
    me_e, me_l = lax.axis_index("elem"), lax.axis_index("lev")
    right, left = lax.rem(me_e + 1, ne), lax.rem(me_e + ne - 1, ne)
    halves = nelem * levels // LANES
    each = nelem // halves
    lrounds = [1 << j for j in range(int(math.log2(nl)))]
    erounds = [1 << j for j in range(int(math.log2(ne)) - 1)]

    loads = [pltpu.make_async_copy(x_hbm.at[:, c], tab.at[c, pl.ds(0, nelem)], in_sem.at[c]) for c in range(chunks)]

    fetch = [pltpu.make_async_copy(a, b, small.at[i]) for i, (a, b) in enumerate(
        [(req_hbm, req_ref), (reft_hbm, reft_ref), (src_hbm, src_ref), (tm_hbm, tm_ref)])]

    def hello(sem, e, l):
        pl.semaphore_signal(sem, inc=1, device_id=(e, l), device_id_type=MESH)

    barrier = pltpu.get_barrier_semaphore()
    hello(barrier, right, me_l)
    hello(barrier, left, me_l)
    for d in lrounds:
        hello(barrier, me_e, me_l ^ d)
    for copy in fetch + loads:
        copy.start()
    fetch[0].wait()
    pl.semaphore_wait(barrier, 2 + len(lrounds))

    def remote(src, dst, ssem, rsem, e, l):
        return pltpu.make_async_remote_copy(
            src_ref=src, dst_ref=dst, send_sem=ssem, recv_sem=rsem, device_id=(e, l), device_id_type=MESH
        )

    ask_l = remote(req_ref, req_r, rq_send.at[0], rq_recv.at[0], left, me_l)
    ask_r = remote(req_ref, req_l, rq_send.at[1], rq_recv.at[1], right, me_l)
    ask_l.start()
    ask_r.start()

    steps = []
    for j, d in enumerate(erounds):
        fwd, back = lax.rem(me_e + d, ne), lax.rem(me_e + ne - d, ne)
        steps.append((lambda j=j, f=fwd, b=back: (hello(e_sem.at[j], f, me_l), hello(e_sem.at[j], b, me_l)),
                      lambda j=j: pl.semaphore_wait(e_sem.at[j], 2)))
    for j, d in enumerate(lrounds):
        steps.append((lambda j=j, d=d: hello(l_sem.at[j], me_e, me_l ^ d),
                      lambda j=j: pl.semaphore_wait(l_sem.at[j], 1)))
    steps[0][0]()

    lane = lax.broadcasted_iota(jnp.int32, (8, LANES), 1)
    point = lane % NPTS
    hi, lo = point // 4, point % 4

    fetch[1].wait()
    refs_f = reft_ref[...].astype(jnp.float32)
    rep = (lax.broadcasted_iota(jnp.int32, (nelem, nelem * levels), 1) // levels
           == lax.broadcasted_iota(jnp.int32, (nelem, nelem * levels), 0)).astype(jnp.float32)
    spread = jnp.dot(refs_f, rep, preferred_element_type=jnp.float32)
    for h in range(halves):
        r = spread[:, h * LANES : (h + 1) * LANES]
        a = jnp.floor((r + 0.5) * (1.0 / SIDE))
        b = r - SIDE * a
        la = basis(-1.0 + a * (2.0 / (SIDE - 1)))
        lb = basis(-1.0 + b * (2.0 / (SIDE - 1)))
        for n in range(NPTS):
            coef[h, n] = la[n // 4] * lb[n % 4]

    if len(steps) > 1:
        steps[0][1]()
        steps[1][0]()
    at = 1

    fetch[2].wait()
    fetch[3].wait()
    ask_l.wait()
    ask_r.wait()
    for load in loads:
        load.wait()
    wanted = [[jnp.maximum(req_r[0, s], 0) for s in range(slots)], [jnp.maximum(req_l[1, s], 0) for s in range(slots)]]

    def rows_to(c, side):
        to = left if side else right
        return remote(sendb.at[c, side], halo.at[c, side], h_send.at[c, side], h_recv.at[c, side], to, me_l)

    for c in range(chunks):
        for side in range(2):
            for s in range(slots):
                sendb[c, side, s] = tab[c, wanted[side][s]]
            rows_to(c, side).start()

    while at < len(steps) - 2:
        steps[at][1]()
        steps[at + 1][0]()
        at += 1

    index = [lane ^ k for k in range(NPTS)]
    row = lax.broadcasted_iota(jnp.int32, (8, LANES), 0)

    def work(c, part):
        for side in range(2):
            rows_to(c, side).wait_recv()
            tab[c, pl.ds(nelem + side * slots, slots)] = halo[c, side]
        total = jnp.zeros((LANES, LANES), jnp.float32)
        for h in range(halves):
            for q in range(each):
                gbuf[h, q * levels : (q + 1) * levels] = tab[c, src_ref[h * each + q]]
            turned[h] = gbuf[h].T
            done = []
            for t in range(LANES // NPTS):
                v = turned[h, t * NPTS : (t + 1) * NPTS]
                low, high = jnp.min(v, axis=0, keepdims=True), jnp.max(v, axis=0, keepdims=True)
                out = jnp.zeros((NPTS, LANES), jnp.float32)
                for n in range(NPTS):
                    out = out + coef[h, n] * turned[h, t * NPTS + n : t * NPTS + n + 1]
                done.append(jnp.minimum(jnp.maximum(out, low), high))
            back = jnp.concatenate(done, axis=0).T
            clip_out[h * each : (h + 1) * each, c] = back.reshape(each, levels, LANES)
            total = total + back

        @pl.when(c == 0)
        def _():
            steps[-2][1]()
            steps[-1][0]()

        return jnp.where(row == c, jnp.sum(total, axis=0, keepdims=True), part)

    part = lax.fori_loop(0, chunks, work, jnp.zeros((8, LANES), jnp.float32))

    edge = [1.0 / 6.0, 5.0 / 6.0]
    weight = jnp.where((hi == 0) | (hi == 3), edge[0], edge[1]) * jnp.where((lo == 0) | (lo == 3), edge[0], edge[1])
    steps[-1][1]()
    part = part * weight
    for k in (1, 2, 4, 8):
        part = part + permute(part, index[k])
    packed = jnp.sum(jnp.where(point == row, part, 0.0), axis=0, keepdims=True)
    massb[0] = packed

    count = ne * nl

    def tell(de):
        e = lax.rem(me_e + de, ne)
        for dl in range(nl):
            l = lax.rem(me_l + dl, nl)
            slot = de * nl + dl - 1
            if isinstance(de, int) and slot < 0:
                continue
            remote(massb.at[0], mrecv.at[slot], m_send, m_recv, e, l).start()

    def tell_loop(de, carry):
        tell(de)
        return carry

    if count <= 64:
        for de in range(ne):
            tell(de)
    else:
        tell(0)
        lax.fori_loop(1, ne, tell_loop, 0)

    tm = jnp.zeros((8, LANES), jnp.float32)
    group = row * (LANES // NPTS) + lane // NPTS
    for t in range(chunks * LANES // NPTS):
        tm = jnp.where(group == t, tm_ref[t], tm)
    tm = tm * (4.0 * nelem * ne * levels * nl)
    for c in range(chunks):
        for side in range(2):
            rows_to(c, side).wait_send()
    everyone = remote(mrecv, mrecv, m_send, m_recv, right, me_l)
    everyone.wait_recv()
    mass = packed
    if count <= 64:
        for s in range(count - 1):
            mass = mass + mrecv[s]
    else:
        mass = lax.fori_loop(0, count - 1, lambda s, m: m + mrecv[s], mass)
    full = permute(jnp.broadcast_to(mass, (8, LANES)), (lane // NPTS) * NPTS + row)
    fac_out[...] = tm / full
    everyone.wait_send()


def per_device(ne, nl, tracers, ref_index, requests, source, target_mean):
    nelem, levels, width = tracers.shape
    chunks = width // LANES
    slots = requests.shape[2]
    x = tracers.reshape(nelem, levels, chunks, LANES).transpose(0, 2, 1, 3)
    f32 = jnp.float32
    vm = lambda *s: pltpu.VMEM(s, f32)
    dma = lambda *s: pltpu.SemaphoreType.DMA(s)
    hbm, vmem = (pl.BlockSpec(memory_space=m) for m in (pltpu.HBM, pltpu.VMEM))
    clipped, factor = pl.pallas_call(
        functools.partial(kernel, ne, nl, nelem, levels, chunks, slots),
        out_shape=(jax.ShapeDtypeStruct((nelem, chunks, levels, LANES), f32), jax.ShapeDtypeStruct((8, LANES), f32)),
        in_specs=[hbm] * 5,
        out_specs=(vmem, vmem),
        scratch_shapes=[
            pltpu.VMEM((NPTS, nelem), jnp.int32),
            pltpu.SMEM((2, slots), jnp.int32),
            pltpu.SMEM((nelem,), jnp.int32),
            pltpu.SMEM((chunks * LANES // NPTS,), f32),
            vm(chunks, nelem + 2 * slots, levels, LANES),
            vm(chunks, 2, slots, levels, LANES),
            vm(chunks, 2, slots, levels, LANES),
            vm(nelem * levels // LANES, LANES, LANES),
            vm(nelem * levels // LANES, LANES, LANES),
            vm(nelem * levels // LANES, NPTS, NPTS, LANES),
            vm(1, 1, LANES),
            vm(ne * nl - 1, 1, LANES),
            pltpu.SMEM((2, slots), jnp.int32),
            pltpu.SMEM((2, slots), jnp.int32),
            dma(chunks), dma(4), dma(2), dma(2), dma(chunks, 2), dma(chunks, 2),
            pltpu.SemaphoreType.DMA, pltpu.SemaphoreType.DMA,
            pltpu.SemaphoreType.REGULAR((max(int(math.log2(ne)) - 1, 1),)),
            pltpu.SemaphoreType.REGULAR((max(int(math.log2(nl)), 1),)),
        ],
        compiler_params=pltpu.CompilerParams(collective_id=0, has_side_effects=True, vmem_limit_bytes=55_600_000),
    )(x, ref_index.T, requests[0], source, target_mean)
    out = clipped * factor[:chunks][None, :, None, :]
    return out.transpose(0, 2, 1, 3).reshape(nelem, levels, width)


def solution(mesh):
    placed = (P("elem", "lev", None), P("elem", None), P("elem", None, None), P("elem"), P())
    return jax.shard_map(
        functools.partial(per_device, mesh.shape["elem"], mesh.shape["lev"]),
        mesh=mesh, in_specs=placed, out_specs=P("elem", "lev", None), check_vma=False,
    )
```

```python
import functools
import math

import jax
import jax.numpy as jnp
from jax import lax
from jax.experimental import pallas as pl
from jax.experimental.pallas import tpu as pltpu
from jax.sharding import PartitionSpec as P

NPTS = 16
SIDE = 8
LANES = 128
MESH = pl.DeviceIdType.MESH
NODES = [-1.0, -math.sqrt(0.2), math.sqrt(0.2), 1.0]


def basis(x):
    d = [x - g for g in NODES]
    scale = [1.0 / math.prod(NODES[i] - NODES[k] for k in range(4) if k != i) for i in range(4)]
    low, high = d[0] * d[1], d[2] * d[3]
    parts = [d[1] * high, d[0] * high, low * d[3], low * d[2]]
    return [p * s for p, s in zip(parts, scale)]


def permute(v, index):
    return jnp.take_along_axis(v, index, axis=1, mode="promise_in_bounds")


def kernel(ne, nl, nelem, levels, chunks, slots, *refs):
    x_hbm, reft_hbm, req_hbm, src_hbm, tm_hbm, clip_out, fac_out = refs[:7]
    (reft_ref, req_ref, src_ref, tm_ref, tab, sendb, halo, gbuf, turned, coef, massb, mrecv, req_r, req_l,
     in_sem, small, rq_send, rq_recv, h_send, h_recv, m_send, m_recv, e_sem, l_sem) = refs[7:]
    me_e, me_l = lax.axis_index("elem"), lax.axis_index("lev")
    right, left = lax.rem(me_e + 1, ne), lax.rem(me_e + ne - 1, ne)
    halves = nelem * levels // LANES
    each = nelem // halves
    lrounds = [1 << j for j in range(int(math.log2(nl)))]
    erounds = [1 << j for j in range(int(math.log2(ne)) - 1)]

    loads = [pltpu.make_async_copy(x_hbm.at[:, c], tab.at[c, pl.ds(0, nelem)], in_sem.at[c]) for c in range(chunks)]

    fetch = [pltpu.make_async_copy(a, b, small.at[i]) for i, (a, b) in enumerate(
        [(req_hbm, req_ref), (reft_hbm, reft_ref), (src_hbm, src_ref), (tm_hbm, tm_ref)])]

    def hello(sem, e, l):
        pl.semaphore_signal(sem, inc=1, device_id=(e, l), device_id_type=MESH)

    barrier = pltpu.get_barrier_semaphore()
    hello(barrier, right, me_l)
    hello(barrier, left, me_l)
    for d in lrounds:
        hello(barrier, me_e, me_l ^ d)
    for copy in fetch + loads:
        copy.start()
    fetch[0].wait()
    pl.semaphore_wait(barrier, 2 + len(lrounds))

    def remote(src, dst, ssem, rsem, e, l):
        return pltpu.make_async_remote_copy(
            src_ref=src, dst_ref=dst, send_sem=ssem, recv_sem=rsem, device_id=(e, l), device_id_type=MESH
        )

    ask_l = remote(req_ref, req_r, rq_send.at[0], rq_recv.at[0], left, me_l)
    ask_r = remote(req_ref, req_l, rq_send.at[1], rq_recv.at[1], right, me_l)
    ask_l.start()
    ask_r.start()

    steps = []
    for j, d in enumerate(erounds):
        fwd, back = lax.rem(me_e + d, ne), lax.rem(me_e + ne - d, ne)
        steps.append((lambda j=j, f=fwd, b=back: (hello(e_sem.at[j], f, me_l), hello(e_sem.at[j], b, me_l)),
                      lambda j=j: pl.semaphore_wait(e_sem.at[j], 2)))
    for j, d in enumerate(lrounds):
        steps.append((lambda j=j, d=d: hello(l_sem.at[j], me_e, me_l ^ d),
                      lambda j=j: pl.semaphore_wait(l_sem.at[j], 1)))
    steps[0][0]()

    lane = lax.broadcasted_iota(jnp.int32, (8, LANES), 1)
    point = lane % NPTS
    hi, lo = point // 4, point % 4

    fetch[1].wait()
    refs_f = reft_ref[...].astype(jnp.float32)
    rep = (lax.broadcasted_iota(jnp.int32, (nelem, nelem * levels), 1) // levels
           == lax.broadcasted_iota(jnp.int32, (nelem, nelem * levels), 0)).astype(jnp.float32)
    spread = jnp.dot(refs_f, rep, preferred_element_type=jnp.float32)
    for h in range(halves):
        r = spread[:, h * LANES : (h + 1) * LANES]
        a = jnp.floor((r + 0.5) * (1.0 / SIDE))
        b = r - SIDE * a
        la = basis(-1.0 + a * (2.0 / (SIDE - 1)))
        lb = basis(-1.0 + b * (2.0 / (SIDE - 1)))
        for n in range(NPTS):
            coef[h, n] = la[n // 4] * lb[n % 4]

    if len(steps) > 1:
        steps[0][1]()
        steps[1][0]()
    at = 1

    fetch[2].wait()
    fetch[3].wait()
    ask_l.wait()
    ask_r.wait()
    for load in loads:
        load.wait()
    wanted = [[jnp.maximum(req_r[0, s], 0) for s in range(slots)], [jnp.maximum(req_l[1, s], 0) for s in range(slots)]]

    def rows_to(c, side):
        to = left if side else right
        return remote(sendb.at[c, side], halo.at[c, side], h_send.at[c, side], h_recv.at[c, side], to, me_l)

    for c in range(chunks):
        for side in range(2):
            for s in range(slots):
                sendb[c, side, s] = tab[c, wanted[side][s]]
            rows_to(c, side).start()

    while at < len(steps) - 2:
        steps[at][1]()
        steps[at + 1][0]()
        at += 1

    index = [lane ^ k for k in range(NPTS)]
    row = lax.broadcasted_iota(jnp.int32, (8, LANES), 0)

    def work(c, part):
        for side in range(2):
            rows_to(c, side).wait_recv()
            tab[c, pl.ds(nelem + side * slots, slots)] = halo[c, side]
        total = jnp.zeros((LANES, LANES), jnp.float32)
        for h in range(halves):
            for q in range(each):
                gbuf[h, q * levels : (q + 1) * levels] = tab[c, src_ref[h * each + q]]
            turned[h] = gbuf[h].T
            done = []
            for t in range(LANES // NPTS):
                v = turned[h, t * NPTS : (t + 1) * NPTS]
                low, high = jnp.min(v, axis=0, keepdims=True), jnp.max(v, axis=0, keepdims=True)
                out = jnp.zeros((NPTS, LANES), jnp.float32)
                for n in range(NPTS):
                    out = out + coef[h, n] * turned[h, t * NPTS + n : t * NPTS + n + 1]
                done.append(jnp.minimum(jnp.maximum(out, low), high))
            back = jnp.concatenate(done, axis=0).T
            clip_out[h * each : (h + 1) * each, c] = back.reshape(each, levels, LANES)
            total = total + back

        @pl.when(c == 0)
        def _():
            steps[-2][1]()
            steps[-1][0]()

        return jnp.where(row == c, jnp.sum(total, axis=0, keepdims=True), part)

    part = lax.fori_loop(0, chunks, work, jnp.zeros((8, LANES), jnp.float32))

    edge = [1.0 / 6.0, 5.0 / 6.0]
    weight = jnp.where((hi == 0) | (hi == 3), edge[0], edge[1]) * jnp.where((lo == 0) | (lo == 3), edge[0], edge[1])
    steps[-1][1]()
    part = part * weight
    for k in (1, 2, 4, 8):
        part = part + permute(part, index[k])
    packed = jnp.sum(jnp.where(point == row, part, 0.0), axis=0, keepdims=True)
    massb[0] = packed

    count = ne * nl

    def tell(de):
        e = lax.rem(me_e + de, ne)
        for dl in reversed(range(nl)):
            l = lax.rem(me_l + dl, nl)
            slot = de * nl + dl - 1
            if isinstance(de, int) and slot < 0:
                continue
            remote(massb.at[0], mrecv.at[slot], m_send, m_recv, e, l).start()

    def tell_loop(de, carry):
        tell(de)
        return carry

    if count <= 64:
        for de in sorted(range(ne), key=lambda d: -min(d, ne - d)):
            tell(de)
    else:
        tell(0)
        lax.fori_loop(1, ne, tell_loop, 0)

    tm = jnp.zeros((8, LANES), jnp.float32)
    group = row * (LANES // NPTS) + lane // NPTS
    for t in range(chunks * LANES // NPTS):
        tm = jnp.where(group == t, tm_ref[t], tm)
    tm = tm * (4.0 * nelem * ne * levels * nl)
    for c in range(chunks):
        for side in range(2):
            rows_to(c, side).wait_send()
    everyone = remote(mrecv, mrecv, m_send, m_recv, right, me_l)
    everyone.wait_recv()
    mass = packed
    if count <= 64:
        for s in range(count - 1):
            mass = mass + mrecv[s]
    else:
        mass = lax.fori_loop(0, count - 1, lambda s, m: m + mrecv[s], mass)
    full = permute(jnp.broadcast_to(mass, (8, LANES)), (lane // NPTS) * NPTS + row)
    fac_out[...] = tm / full
    everyone.wait_send()


def per_device(ne, nl, tracers, ref_index, requests, source, target_mean):
    nelem, levels, width = tracers.shape
    chunks = width // LANES
    slots = requests.shape[2]
    x = tracers.reshape(nelem, levels, chunks, LANES).transpose(0, 2, 1, 3)
    f32 = jnp.float32
    vm = lambda *s: pltpu.VMEM(s, f32)
    dma = lambda *s: pltpu.SemaphoreType.DMA(s)
    hbm, vmem = (pl.BlockSpec(memory_space=m) for m in (pltpu.HBM, pltpu.VMEM))
    clipped, factor = pl.pallas_call(
        functools.partial(kernel, ne, nl, nelem, levels, chunks, slots),
        out_shape=(jax.ShapeDtypeStruct((nelem, chunks, levels, LANES), f32), jax.ShapeDtypeStruct((8, LANES), f32)),
        in_specs=[hbm] * 5,
        out_specs=(vmem, vmem),
        scratch_shapes=[
            pltpu.VMEM((NPTS, nelem), jnp.int32),
            pltpu.SMEM((2, slots), jnp.int32),
            pltpu.SMEM((nelem,), jnp.int32),
            pltpu.SMEM((chunks * LANES // NPTS,), f32),
            vm(chunks, nelem + 2 * slots, levels, LANES),
            vm(chunks, 2, slots, levels, LANES),
            vm(chunks, 2, slots, levels, LANES),
            vm(nelem * levels // LANES, LANES, LANES),
            vm(nelem * levels // LANES, LANES, LANES),
            vm(nelem * levels // LANES, NPTS, NPTS, LANES),
            vm(1, 1, LANES),
            vm(ne * nl - 1, 1, LANES),
            pltpu.SMEM((2, slots), jnp.int32),
            pltpu.SMEM((2, slots), jnp.int32),
            dma(chunks), dma(4), dma(2), dma(2), dma(chunks, 2), dma(chunks, 2),
            pltpu.SemaphoreType.DMA, pltpu.SemaphoreType.DMA,
            pltpu.SemaphoreType.REGULAR((max(int(math.log2(ne)) - 1, 1),)),
            pltpu.SemaphoreType.REGULAR((max(int(math.log2(nl)), 1),)),
        ],
        compiler_params=pltpu.CompilerParams(collective_id=0, has_side_effects=True, vmem_limit_bytes=55_600_000),
    )(x, ref_index.T, requests[0], source, target_mean)
    out = clipped * factor[:chunks][None, :, None, :]
    return out.transpose(0, 2, 1, 3).reshape(nelem, levels, width)


def solution(mesh):
    placed = (P("elem", "lev", None), P("elem", None), P("elem", None, None), P("elem"), P())
    return jax.shard_map(
        functools.partial(per_device, mesh.shape["elem"], mesh.shape["lev"]),
        mesh=mesh, in_specs=placed, out_specs=P("elem", "lev", None), check_vma=False,
    )
```
